64 devices in a mesh: rep: 8 (over x, y, core), dp: 8 (over z).
Axes of the slice: x: 2, y: 2, z: 8, core: 2. Of those that a mesh axis runs over, the one named last changes fastest.
The devices are a block of a 4x4x8 slice.
Arguments:
- a: bfloat16 [64, 4, 4096, 640], P(('rep', 'dp')), parts along dimension 0
- g: bfloat16 [64, 4, 4096, 2432], P(('rep', 'dp')), parts along dimension 0
Outputs:
- output: bfloat16 [32, 640, 2432], P('rep'), parts along dimension 0
There are 8 independent parts. The reference program is written for one: setup_inputs(seed, part) draws one part's arguments, and reference() takes and returns one part's arrays. A program takes and returns all parts, laid end to end along the dimension named above; each array names one.
All inputs are finite; a program needn't handle non-finite values.
Results may differ from the reference program's by a relative error of at most 0.012.
Values are sent between devices in bfloat16 or wider.
A program may use at most 768 MiB of HBM per device.

```python
import jax
import jax.numpy as jnp
from jax import lax

DEVICES = 8
MATRICES = 4
TOKENS = 4096
D = 640
FF = 2432


def setup_inputs(seed: int = 0, part: int = 0) -> dict:
    ka, kg, ks = (jax.random.fold_in(k, part) for k in jax.random.split(jax.random.key(seed), 3))
    size = 2.0 ** jax.random.uniform(ks, (DEVICES, MATRICES, 1, 1), jnp.float32, -1.0, 1.0)
    a = jax.random.normal(ka, (DEVICES, MATRICES, TOKENS, D), jnp.float32)
    g = size * jax.random.normal(kg, (DEVICES, MATRICES, TOKENS, FF), jnp.float32) * (DEVICES * TOKENS) ** -0.5
    return {"a": a.astype(jnp.bfloat16), "g": g.astype(jnp.bfloat16)}


def reference(a, g):
    def take(so_far, one):
        return so_far + jnp.einsum("ntd,ntf->ndf", *one, preferred_element_type=jnp.float32), None

    return lax.scan(take, jnp.zeros((MATRICES, D, FF), jnp.float32), (a, g))[0].astype(jnp.bfloat16)
```

```python
import functools

import jax
import jax.numpy as jnp
from jax import lax
from jax.experimental import pallas as pl
from jax.experimental.pallas import tpu as pltpu
from jax.sharding import PartitionSpec as P

LANES = 128
WIDE = 2 * LANES
CHUNKS = 4
MESH = pl.DeviceIdType.MESH


def kernel(n, a_ref, g_ref, out_ref, land, a_t, g_buf, part, moving, whole,
           a_sem, g_sem, send_sem, recv_sem, out_sem):
    matrices, tokens, d_model = a_ref.shape
    blocks = g_ref.shape[2] // LANES
    pairs = matrices * blocks // 2
    stages = pairs // 2
    rows = d_model // n
    hold = part.shape[0]
    step_rows = tokens // CHUNKS
    last = 2 * n - 2
    me = lax.axis_index("dp")
    beside = (lax.rem(me + 1, n), lax.rem(me + n - 1, n))

    def owner(d, away):
        sign = 1 - 2 * d
        return lax.rem(me - sign * away + 2 * n, n)

    def at(c):
        return pl.ds(pl.multiple_of(c * rows, rows), rows)

    def a_copy(k):
        slot = lax.rem(k, CHUNKS)
        return pltpu.make_async_copy(
            a_ref.at[k // CHUNKS, pl.ds(pl.multiple_of(slot * step_rows, step_rows), step_rows)],
            land.at[slot], a_sem.at[slot])

    def place(b):
        return b // blocks, pl.multiple_of(lax.rem(b, blocks) * LANES, LANES)

    def crosses(p):
        return lax.rem(2 * p, blocks) == blocks - 1

    def g_copy(p, slot):
        m, col = place(2 * p)
        return pltpu.make_async_copy(
            g_ref.at[m, :, pl.ds(col, WIDE)], g_buf.at[slot], g_sem.at[slot])

    def g_start(p):
        slot = lax.rem(p, 3)

        @pl.when(jnp.logical_not(crosses(p)))
        def _():
            g_copy(p, slot).start()

        @pl.when(crosses(p))
        def _():
            for i in range(2):
                m, col = place(2 * p + i)
                pltpu.make_async_copy(
                    g_ref.at[m, :, pl.ds(col, LANES)],
                    g_buf.at[slot, :, pl.ds(i * LANES, LANES)], g_sem.at[slot]).start()

    def turn(k):
        a_copy(k).wait()
        slot = lax.rem(k, CHUNKS)
        half = step_rows // 2
        for i in range(2):
            a_t[lax.rem(k // CHUNKS, 2), :,
                pl.ds(pl.multiple_of(slot * step_rows + i * half, half), half)] = (
                    land[slot, pl.ds(i * half, half)].T)

        @pl.when(k + CHUNKS < matrices * CHUNKS)
        def _():
            a_copy(k + CHUNKS).start()

    def compute(q, d):
        p = 2 * q + d
        slot = lax.rem(p, 3)
        keep = lax.rem(q, hold)
        pltpu.make_async_copy(
            g_ref.at[0, :, pl.ds(0, WIDE)], g_buf.at[slot], g_sem.at[slot]).wait()

        @pl.when(p + 2 < pairs)
        def _():
            g_start(p + 2)

        first = lax.rem(2 * p // blocks, 2)

        @pl.when(jnp.logical_not(crosses(p)))
        def _():
            part[keep, d] = jnp.dot(
                a_t[first], g_buf[slot], preferred_element_type=jnp.float32)

        @pl.when(crosses(p))
        def _():
            for i in range(2):
                side = pl.ds(i * LANES, LANES)
                part[keep, d, :, side] = jnp.dot(
                    a_t[lax.rem(first + i, 2)], g_buf[slot, :, side],
                    preferred_element_type=jnp.float32)

    def message(q, d, t, source, target, to):
        return pltpu.make_async_remote_copy(
            src_ref=source, dst_ref=target,
            send_sem=send_sem.at[d, q, lax.rem(t, 2)],
            recv_sem=recv_sem.at[d, q, t],
            device_id={"dp": to}, device_id_type=MESH)

    def any_message(q, d, t):
        ref = moving.at[d, q, 0]
        return message(q, d, t, ref, ref, beside[0])

    def begin(q, d):
        c = owner(d, 1)
        to = lax.rem(me + 1 - 2 * d + n, n)
        moving[d, q, 0] = part[lax.rem(q, hold), d, at(c)].astype(jnp.bfloat16)
        message(q, d, 0, moving.at[d, q, 0], moving.at[d, q, 1], to).start()

    def reduce_step(q, t):
        for d in range(2):
            any_message(q, d, t - 1).wait_recv()
            c = owner(d, 1 + t)
            so_far = moving[d, q, t].astype(jnp.float32)
            moving[d, q, t] = (so_far + part[lax.rem(q, hold), d, at(c)]).astype(jnp.bfloat16)

            @pl.when(t >= 2)
            def _():
                any_message(q, d, t).wait_send()

            message(q, d, t, moving.at[d, q, t], moving.at[d, q, t + 1], beside[d]).start()

    def finish_step(q):
        t = n - 1
        for d in range(2):
            any_message(q, d, t - 1).wait_recv()
            so_far = moving[d, q, t].astype(jnp.float32)
            mine = whole.at[2 * q + d, at(me)]
            mine[...] = (so_far + part[lax.rem(q, hold), d, at(me)]).astype(jnp.bfloat16)
            any_message(q, d, t).wait_send()
            message(q, d, t, mine, mine, beside[d]).start()

    def gather_step(q, t):
        for d in range(2):
            any_message(q, d, t - 1).wait_recv()
            block = whole.at[2 * q + d, at(owner(d, t - n + 1))]
            any_message(q, d, t).wait_send()
            message(q, d, t, block, block, beside[d]).start()

    def out_copy(p, i, width):
        m, col = place(2 * p + i)
        return pltpu.make_async_copy(
            whole.at[p, :, pl.ds(i * LANES, width)],
            out_ref.at[m, :, pl.ds(col, width)], out_sem.at[p])

    def close(q):
        for d in range(2):
            p = 2 * q + d
            any_message(q, d, last - 1).wait_recv()
            any_message(q, d, 0).wait_send()
            any_message(q, d, 1).wait_send()

            @pl.when(jnp.logical_not(crosses(p)))
            def _():
                out_copy(p, 0, WIDE).start()

            @pl.when(crosses(p))
            def _():
                for i in range(2):
                    out_copy(p, i, LANES).start()

    for k in range(CHUNKS):
        a_copy(k).start()
    for p in range(2):
        g_start(p)
    barrier = pltpu.get_barrier_semaphore()
    for to in beside:
        pl.semaphore_signal(barrier, inc=1, device_id={"dp": to}, device_id_type=MESH)
    pl.semaphore_wait(barrier, 2)

    def first_chunks(k, _):
        turn(k)
        return 0

    lax.fori_loop(0, CHUNKS, first_chunks, 0)

    def tick(r, _):
        @pl.when(jnp.logical_and(lax.rem(r, 5) != 0, r < 15))
        def _():
            turn(r + 3 - r // 5)

        @pl.when(r < stages)
        def _():
            def one(d, _):
                compute(r, d)
                begin(r, d)
                return 0

            lax.fori_loop(0, 2, one, 0)

        def bounds(lo, hi):
            return jnp.maximum(lo, r - stages + 1), jnp.minimum(hi, r) + 1

        def red(t, _):
            reduce_step(r - t, t)
            return 0

        lax.fori_loop(*bounds(1, n - 2), red, 0)

        @pl.when(jnp.logical_and(r >= n - 1, r - (n - 1) < stages))
        def _():
            finish_step(r - (n - 1))

        def gat(t, _):
            gather_step(r - t, t)
            return 0

        lax.fori_loop(*bounds(n, last - 1), gat, 0)

        @pl.when(jnp.logical_and(r >= last, r - last < stages))
        def _():
            close(r - last)

        return 0

    lax.fori_loop(0, stages + last, tick, 0)

    def drain(p, _):
        pltpu.make_async_copy(
            whole.at[0], out_ref.at[0, :, pl.ds(0, WIDE)], out_sem.at[p]).wait()
        return 0

    lax.fori_loop(0, pairs, drain, 0)


def solution(mesh):
    n = mesh.shape["dp"]

    def local(a, g):
        a, g = a[0], g[0]
        matrices, tokens, d_model = a.shape
        ff = g.shape[2]
        pairs = matrices * ff // WIDE
        stages = pairs // 2
        rows = d_model // n
        steps = 2 * n - 2
        call = pl.pallas_call(
            functools.partial(kernel, n),
            out_shape=jax.ShapeDtypeStruct((matrices, d_model, ff), jnp.bfloat16),
            in_specs=[pl.BlockSpec(memory_space=pl.ANY)] * 2,
            out_specs=pl.BlockSpec(memory_space=pl.ANY),
            scratch_shapes=[
                pltpu.VMEM((CHUNKS, tokens // CHUNKS, d_model), jnp.bfloat16),
                pltpu.VMEM((2, d_model, tokens), jnp.bfloat16),
                pltpu.VMEM((3, tokens, WIDE), jnp.bfloat16),
                pltpu.VMEM((n, 2, d_model, WIDE), jnp.float32),
                pltpu.VMEM((2, stages, n, rows, WIDE), jnp.bfloat16),
                pltpu.VMEM((pairs, d_model, WIDE), jnp.bfloat16),
                pltpu.SemaphoreType.DMA((CHUNKS,)),
                pltpu.SemaphoreType.DMA((3,)),
                pltpu.SemaphoreType.DMA((2, stages, 2)),
                pltpu.SemaphoreType.DMA((2, stages, steps)),
                pltpu.SemaphoreType.DMA((pairs,)),
            ],
            compiler_params=pltpu.CompilerParams(
                collective_id=0, has_side_effects=True, vmem_limit_bytes=67043328),
            cost_estimate=pl.CostEstimate(
                flops=2 * matrices * tokens * d_model * ff,
                bytes_accessed=2 * matrices * (tokens * (d_model + ff) + d_model * ff),
                transcendentals=0),
        )
        return call(a, g)

    return jax.shard_map(
        local, mesh=mesh, in_specs=(P(("rep", "dp")), P(("rep", "dp"))),
        out_specs=P("rep"), check_vma=False)
```

```python
import functools

import jax
import jax.numpy as jnp
from jax import lax
from jax.experimental import pallas as pl
from jax.experimental.pallas import tpu as pltpu
from jax.sharding import PartitionSpec as P

LANES = 128
WIDE = 2 * LANES
CHUNKS = 4
TURNS = (6, 7, 8, 9, 12, 14, 16, 18, 21, 23, 25, 27)
GROUPS = (1, 1, 1, 1, 1, 1, 2, 2, 4, 8, 8, 8)
MESH = pl.DeviceIdType.MESH


def plan(groups, steps, tile=1.8, turn=0.4, lag=1.8, wire=0.44, gap=0.036, depth=4.0):
    now, link, after, order = 0.0, 0.0, [], [[]]
    ends = [sum(groups[:i + 1]) for i in range(len(groups))]
    p, tiles = 0, sum(groups)
    while p < tiles or after:
        ready = [x for x in after if x[0] <= now and (link - now < depth or x[1] == steps)]
        if ready:
            x = min(ready, key=lambda x: (x[1], x[0], x[2]))
            after.remove(x)
            _, t, i = x
            order[-1].append((i, t))
            now += 0.06 + 0.12 * groups[i] * (t <= steps // 2)
            if t < steps:
                link = max(link, now) + groups[i] * wire + gap
                after.append((link + lag, t + 1, i))
        elif p < tiles:
            now += tile + turn * (p in TURNS)
            p += 1
            order.append([])
            if p in ends:
                after.append((now, 0, ends.index(p)))
        else:
            now = min(max(t, link - depth + 1e-6) if s < steps else t for t, s, _ in after)
    return order[1:]


def kernel(n, groups, a_ref, g_ref, whole, land, a_t, g_buf, part,
           a_sem, g_sem, first_sem, send_sem, recv_sem):
    matrices, tokens, d_model = a_ref.shape
    blocks = g_ref.shape[2] // LANES
    pairs = matrices * blocks // 2
    rows = d_model // n
    step_rows = tokens // CHUNKS
    last = 2 * n - 2
    begins = [sum(groups[:i]) for i in range(len(groups))]
    me = lax.axis_index("dp")

    def owner(d, away):
        return lax.rem(me - (1 - 2 * d) * away + 2 * n, n)

    def k_rows(k):
        return pl.ds(pl.multiple_of(lax.rem(k, CHUNKS) * step_rows, step_rows), step_rows)

    def a_copy(k):
        slot = lax.rem(k, CHUNKS)
        return pltpu.make_async_copy(
            a_ref.at[k // CHUNKS, k_rows(k)], land.at[slot], a_sem.at[slot])

    def first_g(k):
        return pltpu.make_async_copy(
            g_ref.at[0, k_rows(k), pl.ds(0, WIDE)], g_buf.at[0, k_rows(k)], first_sem.at[k])

    def place(b):
        return b // blocks, pl.multiple_of(lax.rem(b, blocks) * LANES, LANES)

    def crosses(p):
        return lax.rem(2 * p, blocks) == blocks - 1

    def g_start(p):
        slot = lax.rem(p, 3)

        @pl.when(jnp.logical_not(crosses(p)))
        def _():
            m, col = place(2 * p)
            pltpu.make_async_copy(
                g_ref.at[m, :, pl.ds(col, WIDE)], g_buf.at[slot], g_sem.at[slot]).start()

        @pl.when(crosses(p))
        def _():
            for i in range(2):
                m, col = place(2 * p + i)
                pltpu.make_async_copy(
                    g_ref.at[m, :, pl.ds(col, LANES)],
                    g_buf.at[slot, :, pl.ds(i * LANES, LANES)], g_sem.at[slot]).start()

    def turn(k):
        a_copy(k).wait()
        slot = lax.rem(k, CHUNKS)
        half = step_rows // 2
        for i in range(2):
            a_t[lax.rem(k // CHUNKS, 2), :,
                pl.ds(pl.multiple_of(slot * step_rows + i * half, half), half)] = (
                    land[slot, pl.ds(i * half, half)].T)

    def compute(p):
        slot = lax.rem(p, 3)
        pltpu.make_async_copy(
            g_ref.at[0, :, pl.ds(0, WIDE)], g_buf.at[slot], g_sem.at[slot]).wait()

        @pl.when(p + 2 < pairs)
        def _():
            g_start(p + 2)

        first = lax.rem(2 * p // blocks, 2)

        @pl.when(jnp.logical_not(crosses(p)))
        def _():
            both = jnp.dot(a_t[first], g_buf[slot], preferred_element_type=jnp.float32)
            part[p, 0] = both[:, :LANES]
            part[p, 1] = both[:, LANES:]

        @pl.when(crosses(p))
        def _():
            for i in range(2):
                part[p, i] = jnp.dot(
                    a_t[lax.rem(first + i, 2)], g_buf[slot, :, pl.ds(i * LANES, LANES)],
                    preferred_element_type=jnp.float32)

    def message(i, d, t, block, to):
        return pltpu.make_async_remote_copy(
            src_ref=block, dst_ref=block,
            send_sem=send_sem.at[d, i, t % 2], recv_sem=recv_sem.at[d, i, t],
            device_id={"dp": to}, device_id_type=MESH)

    def carry(i, t):
        q, size = begins[i], groups[i]

        def one(d, _):
            def message_of(s):
                return message(i, d, s, whole.at[d, 0, pl.ds(q, size)], me)

            if t > 0:
                message_of(t - 1).wait_recv()
            c = owner(d, 1 + t if t < n else t - n + 1)
            if t < n:
                mine = pl.ds(pl.multiple_of(c * rows, rows), rows)

                def add(j, _):
                    term = part[q + j, d, mine]
                    if t > 0:
                        term = whole[d, c, q + j].astype(jnp.float32) + term
                    whole[d, c, q + j] = term.astype(jnp.bfloat16)
                    return 0

                lax.fori_loop(0, size, add, 0)
            if t >= 2:
                message_of(t - 2).wait_send()
            if t < last:
                to = lax.rem(me + 1 - 2 * d + n, n)
                message(i, d, t, whole.at[d, c, pl.ds(q, size)], to).start()
            else:
                message_of(t - 1).wait_send()
            return 0

        lax.fori_loop(0, 2, one, 0)

    for k in range(CHUNKS):
        a_copy(k).start()
        first_g(k).start()
    barrier = pltpu.get_barrier_semaphore()
    beside = (lax.rem(me + 1, n), lax.rem(me + n - 1, n))
    for to in beside:
        pl.semaphore_signal(barrier, inc=1, device_id={"dp": to}, device_id_type=MESH)
    part[0] = jnp.zeros(part.shape[1:], jnp.float32)

    def first_tile(k, _):
        turn(k)
        first_g(k).wait()

        @pl.when(lax.rem(k, 2) == 1)
        def _():
            g_start(1 + k // 2)

        both = jnp.dot(a_t[0, :, k_rows(k)], g_buf[0, k_rows(k)],
                       preferred_element_type=jnp.float32)
        part[0, 0] += both[:, :LANES]
        part[0, 1] += both[:, LANES:]
        return 0

    lax.fori_loop(0, CHUNKS, first_tile, 0)
    pl.semaphore_wait(barrier, 2)
    order = plan(groups, last)
    for i, t in order[0]:
        carry(i, t)

    def tile(p, _):
        @pl.when(p <= CHUNKS)
        def _():
            a_copy(CHUNKS + p - 1).start()

        k = CHUNKS + sum((p > x).astype(jnp.int32) for x in TURNS)
        due = functools.reduce(jnp.logical_or, [p == x for x in TURNS])

        @pl.when(due)
        def _():
            turn(k)

            @pl.when(k + CHUNKS < matrices * CHUNKS)
            def _():
                a_copy(k + CHUNKS).start()

        compute(p)
        for x in range(1, pairs - 1):
            if order[x]:
                @pl.when(p == x)
                def _():
                    for i, t in order[x]:
                        carry(i, t)

        return 0

    lax.fori_loop(1, pairs, tile, 0)
    for i, t in order[-1]:
        carry(i, t)


def put(n, whole, out_ref, sem):
    blocks = out_ref.shape[3] // LANES

    def one(p, wait):
        for d in range(2):
            b = 2 * p + d
            col = pl.multiple_of(lax.rem(b, blocks) * LANES, LANES)
            copy = pltpu.make_async_copy(
                whole.at[d, :, p], out_ref.at[b // blocks, :, :, pl.ds(col, LANES)],
                sem.at[d, p])
            copy.wait() if wait else copy.start()
        return 0

    lax.fori_loop(0, whole.shape[2], lambda p, _: one(p, False), 0)
    lax.fori_loop(0, whole.shape[2], lambda p, _: one(p, True), 0)


def solution(mesh):
    n = mesh.shape["dp"]

    def local(a, g):
        a, g = a[0], g[0]
        matrices, tokens, d_model = a.shape
        ff = g.shape[2]
        pairs = matrices * ff // WIDE
        rows = d_model // n
        whole = pl.pallas_call(
            functools.partial(kernel, n, GROUPS),
            out_shape=pltpu.VMEM((2, n, pairs, rows, LANES), jnp.bfloat16),
            in_specs=[pl.BlockSpec(memory_space=pl.ANY)] * 2,
            out_specs=pl.BlockSpec(memory_space=pltpu.VMEM),
            scratch_shapes=[
                pltpu.VMEM((CHUNKS, tokens // CHUNKS, d_model), jnp.bfloat16),
                pltpu.VMEM((2, d_model, tokens), jnp.bfloat16),
                pltpu.VMEM((3, tokens, WIDE), jnp.bfloat16),
                pltpu.VMEM((pairs, 2, d_model, LANES), jnp.float32),
                pltpu.SemaphoreType.DMA((CHUNKS,)),
                pltpu.SemaphoreType.DMA((3,)),
                pltpu.SemaphoreType.DMA((CHUNKS,)),
                pltpu.SemaphoreType.DMA((2, len(GROUPS), 2)),
                pltpu.SemaphoreType.DMA((2, len(GROUPS), 2 * n - 2)),
            ],
            compiler_params=pltpu.CompilerParams(
                collective_id=0, has_side_effects=True, vmem_limit_bytes=50 << 20),
            cost_estimate=pl.CostEstimate(
                flops=2 * matrices * tokens * d_model * ff,
                bytes_accessed=2 * matrices * tokens * (d_model + ff),
                transcendentals=0),
        )(a, g)
        out = pl.pallas_call(
            functools.partial(put, n),
            out_shape=jax.ShapeDtypeStruct((matrices, n, rows, ff), jnp.bfloat16),
            in_specs=[pl.BlockSpec(memory_space=pltpu.VMEM)],
            out_specs=pl.BlockSpec(memory_space=pl.ANY),
            scratch_shapes=[pltpu.SemaphoreType.DMA((2, pairs))],
            compiler_params=pltpu.CompilerParams(vmem_limit_bytes=16 << 20),
        )(whole)
        return out.reshape(matrices, d_model, ff)

    return jax.shard_map(
        local, mesh=mesh, in_specs=(P(("rep", "dp")), P(("rep", "dp"))),
        out_specs=P("rep"), check_vma=False)
```

```python
import functools

import jax
import jax.numpy as jnp
from jax import lax
from jax.experimental import pallas as pl
from jax.experimental.pallas import tpu as pltpu
from jax.sharding import PartitionSpec as P

LANES = 128
WIDE = 2 * LANES
CHUNKS = 4
TURNS = (6, 7, 8, 9, 12, 14, 16, 18, 21, 23, 25, 27)
GROUPS = (1, 1, 1, 1, 1, 1, 2, 2, 4, 8, 8, 8)
FRONT = 6
MESH = pl.DeviceIdType.MESH


def plan(groups, n, work=0.6, half=1.0, turn=0.36, load=0.66, lag=1.5, wire=0.44, gap=0.03,
         depth=4.0):
    steps = 2 * n - 2
    ends = [sum(groups[:i + 1]) for i in range(len(groups))]
    rounds = n // 2
    pieces = [(r, p) for r in range(rounds) for p in range(FRONT)]
    pieces += [(h, p) for p in range(FRONT, ends[-1]) for h in range(2)]
    now, link, after, order, done = 0.0, 0.0, [], [], [0] * FRONT
    held = {}
    x = 0
    while x < len(pieces) or after:
        ready = [e for e in after if e[0] <= now and (link - now < depth or e[1] == steps)
                 and not (e[2] < FRONT and e[1] < n and need(e[1], n) >= done[e[2]])]
        if ready:
            e = min(ready, key=lambda e: (e[1], e[0], e[2]))
            after.remove(e)
            _, t, i = e
            order[-1].append((i, t))
            now += 0.06 + 0.08 * groups[i] * (t < n)
            if t < steps:
                link = max(link, now) + groups[i] * wire + gap
                after.append((link + lag, t + 1, i))
        elif x < len(pieces):
            r, p = pieces[x]
            if p < FRONT:
                now = max(now, load * p) + work
                done[p] = r + 1
                if r == 0:
                    after.append((now, 0, p))
            else:
                now += half + turn * (p in TURNS and r == 0)
                if r == 1 and p + 1 in ends:
                    after.append((now, 0, ends.index(p + 1)))
            x += 1
            order.append([])
        else:
            now = min(max(t, link - depth + 1e-6) if s < steps else t for t, s, _ in after)
    return order


def need(t, n):
    away = min(1 + t, n - 1 - t)
    return away - 1 if 0 < away < n // 2 else n // 2 - 1


def kernel(n, groups, a_ref, g_ref, whole, land, a_t, g_buf, part,
           a_sem, g_sem, send_sem, recv_sem):
    matrices, tokens, d_model = a_ref.shape
    blocks = g_ref.shape[2] // LANES
    pairs = matrices * blocks // 2
    rows = d_model // n
    step_rows = tokens // CHUNKS
    last = 2 * n - 2
    begins = [sum(groups[:i]) for i in range(len(groups))]
    me = lax.axis_index("dp")

    def owner(d, away):
        return lax.rem(me - (1 - 2 * d) * away + 2 * n, n)

    def k_rows(k):
        return pl.ds(pl.multiple_of(lax.rem(k, CHUNKS) * step_rows, step_rows), step_rows)

    def a_copy(k):
        slot = lax.rem(k, CHUNKS)
        return pltpu.make_async_copy(
            a_ref.at[k // CHUNKS, k_rows(k)], land.at[slot], a_sem.at[slot])

    def place(b):
        return b // blocks, pl.multiple_of(lax.rem(b, blocks) * LANES, LANES)

    def crosses(p):
        return lax.rem(2 * p, blocks) == blocks - 1

    def g_start(p):
        slot = lax.rem(p, FRONT)

        @pl.when(jnp.logical_not(crosses(p)))
        def _():
            m, col = place(2 * p)
            pltpu.make_async_copy(
                g_ref.at[m, :, pl.ds(col, WIDE)], g_buf.at[slot], g_sem.at[slot]).start()

        @pl.when(crosses(p))
        def _():
            for i in range(2):
                m, col = place(2 * p + i)
                pltpu.make_async_copy(
                    g_ref.at[m, :, pl.ds(col, LANES)],
                    g_buf.at[slot, :, pl.ds(i * LANES, LANES)], g_sem.at[slot]).start()

    def turn(k):
        a_copy(k).wait()
        slot = lax.rem(k, CHUNKS)
        half = step_rows // 2
        for i in range(2):
            a_t[lax.rem(k // CHUNKS, 2), :,
                pl.ds(pl.multiple_of(slot * step_rows + i * half, half), half)] = (
                    land[slot, pl.ds(i * half, half)].T)

    def g_wait(p):
        slot = lax.rem(p, FRONT)
        pltpu.make_async_copy(
            g_ref.at[0, :, pl.ds(0, WIDE)], g_buf.at[slot], g_sem.at[slot]).wait()

    def at(c):
        return pl.ds(pl.multiple_of(c * rows, rows), rows)

    def front(r, p):
        end = r == n // 2 - 1
        ones = (owner(0, 1 + r), jnp.where(end, me, owner(1, 1 + r)))
        left = jnp.concatenate([a_t[0, at(c)] for c in ones], axis=0)
        both = jnp.dot(left, g_buf[p], preferred_element_type=jnp.float32)
        for i, c in enumerate(ones):
            for d in range(2):
                part[p, d, at(c)] = both[i * rows:(i + 1) * rows, d * LANES:(d + 1) * LANES]

    def compute(p, h):
        slot = lax.rem(p, FRONT)
        first = lax.rem(2 * p // blocks, 2)
        some = pl.ds(pl.multiple_of(h * (d_model // 2), d_model // 2), d_model // 2)

        @pl.when(jnp.logical_not(crosses(p)))
        def _():
            both = jnp.dot(a_t[first, some], g_buf[slot], preferred_element_type=jnp.float32)
            part[p, 0, some] = both[:, :LANES]
            part[p, 1, some] = both[:, LANES:]

        @pl.when(crosses(p))
        def _():
            for i in range(2):
                part[p, i, some] = jnp.dot(
                    a_t[lax.rem(first + i, 2), some], g_buf[slot, :, pl.ds(i * LANES, LANES)],
                    preferred_element_type=jnp.float32)

    def message(i, d, t, block, to):
        return pltpu.make_async_remote_copy(
            src_ref=block, dst_ref=block,
            send_sem=send_sem.at[d, i, t % 2], recv_sem=recv_sem.at[d, i, t],
            device_id={"dp": to}, device_id_type=MESH)

    def carry(i, t):
        q, size = begins[i], groups[i]

        def one(d, _):
            def message_of(s):
                return message(i, d, s, whole.at[d, 0, pl.ds(q, size)], me)

            if t > 0:
                message_of(t - 1).wait_recv()
            c = owner(d, 1 + t if t < n else t - n + 1)
            if t < n:
                def add(j, _):
                    term = part[q + j, d, at(c)]
                    if t > 0:
                        term = whole[d, c, q + j].astype(jnp.float32) + term
                    whole[d, c, q + j] = term.astype(jnp.bfloat16)
                    return 0

                lax.fori_loop(0, size, add, 0)
            if t >= 2:
                message_of(t - 2).wait_send()
            if t < last:
                to = lax.rem(me + 1 - 2 * d + n, n)
                message(i, d, t, whole.at[d, c, pl.ds(q, size)], to).start()
            else:
                message_of(t - 1).wait_send()
            return 0

        lax.fori_loop(0, 2, one, 0)

    for k in range(CHUNKS):
        a_copy(k).start()
    g_start(0)
    barrier = pltpu.get_barrier_semaphore()
    beside = (lax.rem(me + 1, n), lax.rem(me + n - 1, n))
    for to in beside:
        pl.semaphore_signal(barrier, inc=1, device_id={"dp": to}, device_id_type=MESH)

    def first_matrix(k, _):
        turn(k)

        @pl.when(k >= CHUNKS - 2)
        def _():
            g_start(1 + k - (CHUNKS - 2))

        return 0

    lax.fori_loop(0, CHUNKS, first_matrix, 0)
    pl.semaphore_wait(barrier, 2)
    order = plan(groups, n)
    early = n // 2 * FRONT

    def follow(x, lo, hi):
        if hi - lo == 1:
            for i, t in order[lo]:
                carry(i, t)
        elif any(order[lo:hi]):
            mid = (lo + hi) // 2

            @pl.when(x < mid)
            def _():
                follow(x, lo, mid)

            @pl.when(x >= mid)
            def _():
                follow(x, mid, hi)

    def front_piece(x, _):
        r, p = x // FRONT, lax.rem(x, FRONT)

        @pl.when(r == 0)
        def _():
            g_wait(p)

            @pl.when(p + 3 < FRONT)
            def _():
                g_start(p + 3)

        @pl.when(jnp.logical_and(r == 1, p < CHUNKS))
        def _():
            a_copy(CHUNKS + p).start()

        front(r, p)

        @pl.when(jnp.logical_and(r == n // 2 - 1, p < FRONT - 1))
        def _():
            g_start(FRONT + p)

        follow(x, 0, early)
        return 0

    lax.fori_loop(0, early, front_piece, 0)

    def piece(x, _):
        p, h = FRONT + x // 2, lax.rem(x, 2)

        @pl.when(h == 0)
        def _():
            k = CHUNKS + sum((p > y).astype(jnp.int32) for y in TURNS)
            due = functools.reduce(jnp.logical_or, [p == y for y in TURNS])

            @pl.when(due)
            def _():
                turn(k)

                @pl.when(k + CHUNKS < matrices * CHUNKS)
                def _():
                    a_copy(k + CHUNKS).start()

            @pl.when(p + FRONT - 1 < pairs)
            def _():
                g_start(p + FRONT - 1)

            g_wait(p)

        compute(p, h)
        follow(early + x, early, len(order))
        return 0

    late = order[-1]
    order[-1] = []
    lax.fori_loop(0, 2 * (pairs - FRONT), piece, 0)
    for i, t in late:
        carry(i, t)


def put(n, whole, out_ref, sem):
    blocks = out_ref.shape[3] // LANES

    def one(p, wait):
        for d in range(2):
            b = 2 * p + d
            col = pl.multiple_of(lax.rem(b, blocks) * LANES, LANES)
            copy = pltpu.make_async_copy(
                whole.at[d, :, p], out_ref.at[b // blocks, :, :, pl.ds(col, LANES)],
                sem.at[d, p])
            copy.wait() if wait else copy.start()
        return 0

    lax.fori_loop(0, whole.shape[2], lambda p, _: one(p, False), 0)
    lax.fori_loop(0, whole.shape[2], lambda p, _: one(p, True), 0)


def solution(mesh):
    n = mesh.shape["dp"]

    def local(a, g):
        a, g = a[0], g[0]
        matrices, tokens, d_model = a.shape
        ff = g.shape[2]
        pairs = matrices * ff // WIDE
        rows = d_model // n
        whole = pl.pallas_call(
            functools.partial(kernel, n, GROUPS),
            out_shape=pltpu.VMEM((2, n, pairs, rows, LANES), jnp.bfloat16),
            in_specs=[pl.BlockSpec(memory_space=pl.ANY)] * 2,
            out_specs=pl.BlockSpec(memory_space=pltpu.VMEM),
            scratch_shapes=[
                pltpu.VMEM((CHUNKS, tokens // CHUNKS, d_model), jnp.bfloat16),
                pltpu.VMEM((2, d_model, tokens), jnp.bfloat16),
                pltpu.VMEM((FRONT, tokens, WIDE), jnp.bfloat16),
                pltpu.VMEM((pairs, 2, d_model, LANES), jnp.float32),
                pltpu.SemaphoreType.DMA((CHUNKS,)),
                pltpu.SemaphoreType.DMA((FRONT,)),
                pltpu.SemaphoreType.DMA((2, len(GROUPS), 2)),
                pltpu.SemaphoreType.DMA((2, len(GROUPS), 2 * n - 2)),
            ],
            compiler_params=pltpu.CompilerParams(
                collective_id=0, has_side_effects=True, vmem_limit_bytes=52 << 20),
            cost_estimate=pl.CostEstimate(
                flops=2 * matrices * tokens * d_model * ff,
                bytes_accessed=2 * matrices * tokens * (d_model + ff),
                transcendentals=0),
        )(a, g)
        out = pl.pallas_call(
            functools.partial(put, n),
            out_shape=jax.ShapeDtypeStruct((matrices, n, rows, ff), jnp.bfloat16),
            in_specs=[pl.BlockSpec(memory_space=pltpu.VMEM)],
            out_specs=pl.BlockSpec(memory_space=pl.ANY),
            scratch_shapes=[pltpu.SemaphoreType.DMA((2, pairs))],
            compiler_params=pltpu.CompilerParams(vmem_limit_bytes=16 << 20),
        )(whole)
        return out.reshape(matrices, d_model, ff)

    return jax.shard_map(
        local, mesh=mesh, in_specs=(P(("rep", "dp")), P(("rep", "dp"))),
        out_specs=P("rep"), check_vma=False)
```

```python
import functools

import jax
import jax.numpy as jnp
from jax import lax
from jax.experimental import pallas as pl
from jax.experimental.pallas import tpu as pltpu
from jax.sharding import PartitionSpec as P

LANES = 128
WIDE = 2 * LANES
CHUNKS = 4
TURNS = (6, 7, 8, 9, 12, 14, 16, 18, 21, 23, 25, 27)
GROUPS = (1, 1, 1, 1, 1, 1, 2, 2, 4, 8, 8, 8)
FRONT = 6
MESH = pl.DeviceIdType.MESH


def plan(groups, n, work=0.55, half=0.95, turn=0.36, load=0.66, lag=1.5, wire=0.44, gap=0.03,
         depth=4.0):
    steps = 2 * n - 2
    ends = [sum(groups[:i + 1]) for i in range(len(groups))]
    rounds = n // 2
    pieces = [(r, p) for r in range(rounds) for p in range(FRONT)]
    pieces += [(h, p) for p in range(FRONT, ends[-1]) for h in range(2)]
    now, link, after, order, done = 0.0, 0.0, [], [], [0] * FRONT
    x = 0
    while x < len(pieces) or after:
        ready = [e for e in after if e[0] <= now and (link - now < depth or e[1] == steps)
                 and not (e[2] < FRONT and e[1] < n and need(e[1], n) >= done[e[2]])]
        if ready:
            e = min(ready, key=lambda e: (e[1], e[0], e[2]))
            after.remove(e)
            _, t, i = e
            order[-1].append((i, t))
            now += 0.06 + 0.08 * groups[i] * (t < n)
            if t < steps:
                link = max(link, now) + groups[i] * wire + gap
                after.append((link + lag, t + 1, i))
        elif x < len(pieces):
            r, p = pieces[x]
            if p < FRONT:
                now = max(now, load * p) + work
                done[p] = r + 1
                if r == 0:
                    after.append((now, 0, p))
            else:
                now += half + turn * (p in TURNS and r == 0)
                if r == 1 and p + 1 in ends:
                    after.append((now, 0, ends.index(p + 1)))
            x += 1
            order.append([])
        else:
            now = min(max(t, link - depth + 1e-6) if s < steps else t for t, s, _ in after)
    return order


def need(t, n):
    away = min(1 + t, n - 1 - t)
    return away - 1 if 0 < away < n // 2 else n // 2 - 1


def kernel(n, groups, a_ref, g_ref, whole, land, a_t, g_buf, part,
           a_sem, g_sem, send_sem, recv_sem):
    matrices, tokens, d_model = a_ref.shape
    blocks = g_ref.shape[2] // LANES
    pairs = matrices * blocks // 2
    rows = d_model // n
    step_rows = tokens // CHUNKS
    last = 2 * n - 2
    begins = [sum(groups[:i]) for i in range(len(groups))]
    me = lax.axis_index("dp")
    beside = (lax.rem(me + 1, n), lax.rem(me + n - 1, n))

    def owner(d, away):
        return lax.rem(me - (1 - 2 * d) * away + 2 * n, n)

    def k_rows(k):
        return pl.ds(pl.multiple_of(lax.rem(k, CHUNKS) * step_rows, step_rows), step_rows)

    def a_copy(k):
        slot = lax.rem(k, CHUNKS)
        return pltpu.make_async_copy(
            a_ref.at[k // CHUNKS, k_rows(k)], land.at[slot], a_sem.at[slot])

    def place(b):
        return b // blocks, pl.multiple_of(lax.rem(b, blocks) * LANES, LANES)

    def crosses(p):
        return lax.rem(2 * p, blocks) == blocks - 1

    def g_start(p):
        slot = lax.rem(p, FRONT)

        @pl.when(jnp.logical_not(crosses(p)))
        def _():
            m, col = place(2 * p)
            pltpu.make_async_copy(
                g_ref.at[m, :, pl.ds(col, WIDE)], g_buf.at[slot], g_sem.at[slot]).start()

        @pl.when(crosses(p))
        def _():
            for i in range(2):
                m, col = place(2 * p + i)
                pltpu.make_async_copy(
                    g_ref.at[m, :, pl.ds(col, LANES)],
                    g_buf.at[slot, :, pl.ds(i * LANES, LANES)], g_sem.at[slot]).start()

    def turn(k):
        a_copy(k).wait()
        slot = lax.rem(k, CHUNKS)
        half = step_rows // 2
        for i in range(2):
            a_t[lax.rem(k // CHUNKS, 2), :,
                pl.ds(pl.multiple_of(slot * step_rows + i * half, half), half)] = (
                    land[slot, pl.ds(i * half, half)].T)

    def g_wait(p):
        slot = lax.rem(p, FRONT)
        pltpu.make_async_copy(
            g_ref.at[0, :, pl.ds(0, WIDE)], g_buf.at[slot], g_sem.at[slot]).wait()

    def at(c):
        return pl.ds(pl.multiple_of(c * rows, rows), rows)

    def front(r, p):
        end = r == n // 2 - 1
        ones = (owner(0, 1 + r), jnp.where(end, me, owner(1, 1 + r)))
        left = jnp.concatenate([a_t[0, at(c)] for c in ones], axis=0)
        both = jnp.dot(left, g_buf[p], preferred_element_type=jnp.float32)
        for i, c in enumerate(ones):
            for d in range(2):
                part[p, d, at(c)] = both[i * rows:(i + 1) * rows, d * LANES:(d + 1) * LANES]

    def compute(p, h):
        slot = lax.rem(p, FRONT)
        first = lax.rem(2 * p // blocks, 2)
        some = pl.ds(pl.multiple_of(h * (d_model // 2), d_model // 2), d_model // 2)

        @pl.when(jnp.logical_not(crosses(p)))
        def _():
            both = jnp.dot(a_t[first, some], g_buf[slot], preferred_element_type=jnp.float32)
            part[p, 0, some] = both[:, :LANES]
            part[p, 1, some] = both[:, LANES:]

        @pl.when(crosses(p))
        def _():
            for i in range(2):
                part[p, i, some] = jnp.dot(
                    a_t[lax.rem(first + i, 2), some], g_buf[slot, :, pl.ds(i * LANES, LANES)],
                    preferred_element_type=jnp.float32)

    def message(i, d, t, block, to):
        return pltpu.make_async_remote_copy(
            src_ref=block, dst_ref=block,
            send_sem=send_sem.at[d, i, t % 2], recv_sem=recv_sem.at[d, i, t],
            device_id={"dp": to}, device_id_type=MESH)

    def carry(i, t):
        q, size = begins[i], groups[i]
        c = [owner(d, 1 + t if t < n else t - n + 1) for d in range(2)]

        def message_of(d, s):
            return message(i, d, s, whole.at[d, 0, pl.ds(q, size)], me)

        if t > 0:
            for d in range(2):
                message_of(d, t - 1).wait_recv()
        if t < n:
            def add(j, _):
                for d in range(2):
                    term = part[q + j, d, at(c[d])]
                    if t > 0:
                        term = whole[d, c[d], q + j].astype(jnp.float32) + term
                    whole[d, c[d], q + j] = term.astype(jnp.bfloat16)
                return 0

            if size == 1:
                add(0, 0)
            else:
                lax.fori_loop(0, size, add, 0)
        for d in range(2):
            if t >= 2:
                message_of(d, t - 2).wait_send()
            if t < last:
                message(i, d, t, whole.at[d, c[d], pl.ds(q, size)], beside[d]).start()
            else:
                message_of(d, t - 1).wait_send()

    for k in range(CHUNKS):
        a_copy(k).start()
    g_start(0)
    barrier = pltpu.get_barrier_semaphore()
    for to in beside:
        pl.semaphore_signal(barrier, inc=1, device_id={"dp": to}, device_id_type=MESH)

    def first_matrix(k, _):
        turn(k)

        @pl.when(k >= CHUNKS - 2)
        def _():
            g_start(1 + k - (CHUNKS - 2))

        return 0

    lax.fori_loop(0, CHUNKS, first_matrix, 0)
    pl.semaphore_wait(barrier, 2)
    order = plan(groups, n)
    early = n // 2 * FRONT

    def follow(x, lo, hi):
        if hi - lo == 1:
            for i, t in order[lo]:
                carry(i, t)
        elif any(order[lo:hi]):
            mid = (lo + hi) // 2

            @pl.when(x < mid)
            def _():
                follow(x, lo, mid)

            @pl.when(x >= mid)
            def _():
                follow(x, mid, hi)

    def front_piece(x, _):
        r, p = x // FRONT, lax.rem(x, FRONT)

        @pl.when(r == 0)
        def _():
            g_wait(p)

            @pl.when(p + 3 < FRONT)
            def _():
                g_start(p + 3)

        @pl.when(jnp.logical_and(r == 1, p < CHUNKS))
        def _():
            a_copy(CHUNKS + p).start()

        front(r, p)

        @pl.when(jnp.logical_and(r == n // 2 - 1, p < FRONT - 1))
        def _():
            g_start(FRONT + p)

        follow(x, 0, early)
        return 0

    lax.fori_loop(0, early, front_piece, 0)

    def piece(x, _):
        p, h = FRONT + x // 2, lax.rem(x, 2)

        @pl.when(h == 0)
        def _():
            k = CHUNKS + sum((p > y).astype(jnp.int32) for y in TURNS)
            due = functools.reduce(jnp.logical_or, [p == y for y in TURNS])

            @pl.when(due)
            def _():
                turn(k)

                @pl.when(k + CHUNKS < matrices * CHUNKS)
                def _():
                    a_copy(k + CHUNKS).start()

            @pl.when(p + FRONT - 1 < pairs)
            def _():
                g_start(p + FRONT - 1)

            g_wait(p)

        compute(p, h)
        follow(early + x, early, len(order))
        return 0

    late = order[-1]
    order[-1] = []
    lax.fori_loop(0, 2 * (pairs - FRONT), piece, 0)
    for i, t in late:
        carry(i, t)


def put(n, whole, out_ref, sem):
    blocks = out_ref.shape[3] // LANES
    copies = []
    for b in range(2 * whole.shape[2]):
        p, d = divmod(b, 2)
        m, col = divmod(b, blocks)
        copies.append(pltpu.make_async_copy(
            whole.at[d, :, p], out_ref.at[m, :, :, pl.ds(col * LANES, LANES)], sem.at[d, p]))
    for copy in copies:
        copy.start()
    for copy in copies:
        copy.wait()


def solution(mesh):
    n = mesh.shape["dp"]

    def local(a, g):
        a, g = a[0], g[0]
        matrices, tokens, d_model = a.shape
        ff = g.shape[2]
        pairs = matrices * ff // WIDE
        rows = d_model // n
        whole = pl.pallas_call(
            functools.partial(kernel, n, GROUPS),
            out_shape=pltpu.VMEM((2, n, pairs, rows, LANES), jnp.bfloat16),
            in_specs=[pl.BlockSpec(memory_space=pl.ANY)] * 2,
            out_specs=pl.BlockSpec(memory_space=pltpu.VMEM),
            scratch_shapes=[
                pltpu.VMEM((CHUNKS, tokens // CHUNKS, d_model), jnp.bfloat16),
                pltpu.VMEM((2, d_model, tokens), jnp.bfloat16),
                pltpu.VMEM((FRONT, tokens, WIDE), jnp.bfloat16),
                pltpu.VMEM((pairs, 2, d_model, LANES), jnp.float32),
                pltpu.SemaphoreType.DMA((CHUNKS,)),
                pltpu.SemaphoreType.DMA((FRONT,)),
                pltpu.SemaphoreType.DMA((2, len(GROUPS), 2)),
                pltpu.SemaphoreType.DMA((2, len(GROUPS), 2 * n - 2)),
            ],
            compiler_params=pltpu.CompilerParams(
                collective_id=0, has_side_effects=True, vmem_limit_bytes=52 << 20),
            cost_estimate=pl.CostEstimate(
                flops=2 * matrices * tokens * d_model * ff,
                bytes_accessed=2 * matrices * tokens * (d_model + ff),
                transcendentals=0),
        )(a, g)
        out = pl.pallas_call(
            functools.partial(put, n),
            out_shape=jax.ShapeDtypeStruct((matrices, n, rows, ff), jnp.bfloat16),
            in_specs=[pl.BlockSpec(memory_space=pltpu.VMEM)],
            out_specs=pl.BlockSpec(memory_space=pl.ANY),
            scratch_shapes=[pltpu.SemaphoreType.DMA((2, pairs))],
            compiler_params=pltpu.CompilerParams(vmem_limit_bytes=16 << 20),
        )(whole)
        return out.reshape(matrices, d_model, ff)

    return jax.shard_map(
        local, mesh=mesh, in_specs=(P(("rep", "dp")), P(("rep", "dp"))),
        out_specs=P("rep"), check_vma=False)
```
